32 devices in a mesh: blk: 8 (over z, y), batch: 4 (over x, core).
Axes of the slice: x: 2, y: 2, z: 4, core: 2. Of those that a mesh axis runs over, the one named last changes fastest.
Arguments:
- coefficients: bfloat16 [120, 24576], P(None, ('blk', 'batch')), may hold values from -6 to 6
- transforms: bfloat16 [12, 24, 24576], P(None, 'batch', 'blk'), may hold values from -6 to 6
- basis: bfloat16 [120, 3, 4096], P(None, None, 'blk'), may hold values from -0.5 to 0.5
- template: bfloat16 [3, 4096], P(None, 'blk'), may hold values from -6 to 6
- skin_weights: bfloat16 [24, 4096], P(None, 'blk'), may hold values from 0.019897461 to 1
Outputs:
- skinned: bfloat16 [24576, 4, 3, 512], P(('blk', 'batch'))
The draws below stay inside these ranges and needn't reach their ends.
All inputs are finite; a program needn't handle non-finite values.
Results may differ from the reference program's by a relative error of at most 0.0049.
Values may be sent and summed in bfloat16 or wider, within the bound.
A program may use at most 192 MiB of HBM per device.

```python
import math
import jax
import jax.numpy as jnp
from jax import lax

K = 120
J = 24
VB = 512
R = 768
STEPS = 4
VERTS = 4096
CHARS = 24576
N_BLK = 8
N_BATCH = 4


def levels(stream_key, dims, pieces, low, top_value):
    def one(axis_at, parts):
        heights = jax.random.uniform(jax.random.fold_in(jax.random.fold_in(stream_key, 6), axis_at), (parts,), jnp.float32, low / len(pieces), top_value / len(pieces))
        return jnp.repeat(jnp.exp(heights), dims[axis_at] // parts).reshape((-1,) + (1,) * (len(dims) - axis_at - 1))

    gain = one(*pieces[0])
    for cut in pieces[1:]:
        gain = gain * one(*cut)
    return gain


def noise(rng, extent, spread, reach, pieces=(), held_as=jnp.bfloat16):
    entries = jax.random.normal(rng, extent, jnp.float32) * spread
    if len(pieces) > 0:
        entries = levels(rng, extent, pieces, -0.22, 0.18) * entries
    return jnp.clip(entries, min=-reach, max=reach).astype(held_as)


def setup_inputs(seed: int = 0) -> dict:
    keys = jax.random.split(jax.random.key(seed), 6)
    return {
        "coefficients": noise(keys[0], (K, CHARS), 1.0, 6.0, ((1, 32),)),
        "transforms": noise(keys[1], (12, J, CHARS), 1.0, 6.0, ((1, 4), (2, 8))),
        "basis": noise(keys[2], (K, 3, VERTS), K ** -0.5, 0.5, ((2, 8),)),
        "template": noise(keys[3], (3, VERTS), 1.0, 6.0, ((1, 8),)),
        "skin_weights": jnp.clip(jnp.exp(math.log(1.0) - 3.9171631 * jax.random.uniform(keys[4], (J, VERTS), jnp.float32) ** levels(keys[4], (J, VERTS), ((1, 8),), -0.2, 0.2)), 0.019897461, 1.0).astype(jnp.bfloat16),
    }


def skin_block(coefficients, joint_poses, basis_block, template_block, weight_block):
    flattened = basis_block.reshape(basis_block.shape[0], -1)
    shaped = jnp.dot(coefficients.T, flattened, preferred_element_type=jnp.float32)
    shaped = shaped + template_block.reshape(1, -1).astype(jnp.float32)
    shaped = shaped.reshape(coefficients.shape[1], 3, -1)
    blended = jnp.einsum("mjr,jv->mrv", joint_poses.astype(jnp.float32), weight_block.astype(jnp.float32))
    positions = []
    for matrix_row in range(3):
        component = blended[4 * matrix_row + 3]
        for column in range(3):
            component = component + blended[4 * matrix_row + column] * shaped[:, column, :]
        positions.append(component)
    return jnp.stack(positions, axis=1).astype(jnp.bfloat16)


def reference(coefficients, transforms, basis, template, skin_weights):
    weight_float = skin_weights.astype(jnp.float32)
    normalized = (weight_float / jnp.sum(weight_float, axis=0, keepdims=True)).astype(jnp.bfloat16)
    group_size = R * N_BATCH

    def per_group(cycle_group):
        offset = (cycle_group * group_size).astype(jnp.int32)
        group_coefficients = lax.dynamic_slice_in_dim(coefficients, offset, group_size, 1)
        group_poses = lax.dynamic_slice_in_dim(transforms, offset, group_size, 2)
        results = []
        for step_index in range(STEPS):
            block_index = jnp.mod(cycle_group - step_index, N_BLK).astype(jnp.int32)
            vertex_offset = (block_index * VB).astype(jnp.int32)
            basis_block = lax.dynamic_slice_in_dim(basis, vertex_offset, VB, 2)
            template_block = lax.dynamic_slice_in_dim(template, vertex_offset, VB, 1)
            weight_block = lax.dynamic_slice_in_dim(normalized, vertex_offset, VB, 1)
            results.append(skin_block(group_coefficients, group_poses, basis_block, template_block, weight_block))
        return jnp.stack(results, axis=1)

    stacked = lax.map(per_group, jnp.arange(N_BLK, dtype=jnp.int32))
    return stacked.reshape(N_BLK * group_size, STEPS, 3, VB)
```

```python
import functools
import jax
import jax.numpy as jnp
from jax import lax
from jax.experimental import pallas as pl
from jax.experimental.pallas import tpu as pltpu
from jax.sharding import PartitionSpec as P

STEPS = 4
LANES = 128
WIDE = 256
ROWS = 128
SLOT = 8
PITCH = 20
BF16 = jnp.bfloat16
F32 = jnp.float32
LAST = STEPS - 1


def place_weights(raw, n_batch, wv):
    joints, verts = raw.shape
    jl = joints // n_batch
    w = raw[...].astype(F32)
    w = (w / jnp.sum(w, axis=0, keepdims=True)).astype(BF16).astype(F32)
    gap = jnp.zeros((SLOT - jl, verts), F32)
    parts = []
    for i in range(n_batch):
        parts += [w[i * jl:(i + 1) * jl], gap]
    packed = jnp.concatenate(parts, axis=0).astype(BF16)
    span = n_batch * SLOT
    for q in range(4):
        wv[q, q * span:(q + 1) * span, :] = packed


def skin_rows(step, coefs, poses, basis, te, wv, mixed):
    k, verts = basis.shape[1], basis.shape[2]
    co = coefs[:, :k]
    ps = [poses[d] for d in range(3)]
    for n in range(verts // WIDE):
        cols = slice(n * WIDE, (n + 1) * WIDE)
        shaped = [
            jnp.dot(co, basis[e, :, cols], preferred_element_type=F32) + te[e:e + 1, cols].astype(F32)
            for e in range(3)
        ]
        for d in range(3):
            total = jnp.dot(ps[d], wv[3, :, cols], preferred_element_type=F32)
            for e in range(3):
                total = total + shaped[e] * jnp.dot(ps[d], wv[e, :, cols], preferred_element_type=F32)
            for h in range(WIDE // LANES):
                g = (n * (WIDE // LANES) + h) * STEPS + step
                at = 2 * (g % 8) + g // 8
                mixed(d, at, total[:, h * LANES:(h + 1) * LANES])


def front_kernel(
    n_blk, n_batch, co_ref, tr_ref, ba_ref, te_ref, we_ref,
    mix, co_t, po_t, bas, tes, wes,
    cov, stage, trv, wv, tr_send, tr_recv, bl_send, bl_recv, fw_send, fw_recv, own_sem,
):
    blk, bat = lax.axis_index("blk"), lax.axis_index("batch")
    sibling = bat + 1 - 2 * lax.rem(bat, 2)
    odd = lax.rem(blk, 2)
    pair = blk + 1 - 2 * odd
    after = lax.rem(blk + 2, n_blk)
    before = lax.rem(blk + n_blk - 2, n_blk)
    chars = trv.shape[3]
    chunks = chars // ROWS
    comps = trv.shape[1]
    jl = trv.shape[2]
    k = cov.shape[0]
    half = bas.shape[3] // 2

    def rows_of(q, c):
        return pl.ds(pl.multiple_of(q * chars + c * ROWS, LANES), ROWS)

    own = [
        pltpu.make_async_copy(tr_ref, stage, own_sem.at[0]),
        pltpu.make_async_copy(ba_ref, bas.at[0], own_sem.at[1]),
        pltpu.make_async_copy(we_ref, wes.at[0], own_sem.at[2]),
        pltpu.make_async_copy(te_ref, tes.at[0], own_sem.at[3]),
        pltpu.make_async_copy(co_ref, cov, own_sem.at[4]),
        pltpu.make_async_copy(
            tr_ref.at[:, :, pl.ds(pl.multiple_of(bat * chars, LANES), chars)], trv.at[bat], own_sem.at[5]
        ),
    ]
    for c in own:
        c.start()

    partners = [lax.rem(bat + i, n_batch) for i in range(1, n_batch)]
    barrier = pltpu.get_barrier_semaphore()
    for q in partners:
        pl.semaphore_signal(barrier, inc=1, device_id={"blk": blk, "batch": q})
    for b in (pair, after, before):
        pl.semaphore_signal(barrier, inc=1, device_id={"blk": b, "batch": bat})

    wv[...] = jnp.zeros_like(wv)

    mine = pl.ds(pl.multiple_of(lax.rem(bat, 2) * half, LANES), half)
    pieces = [
        [tes, wes, (bas, 0)],
        [(bas, 1)],
        [(bas, 2)],
    ]
    count = len(pieces)

    def part(entry, slot):
        if isinstance(entry, tuple):
            return entry[0].at[slot, entry[1], :, mine]
        return entry.at[slot, :, mine]

    def hop(slot_from, slot_to, piece, where, send, recv, target):
        made = []
        for i, entry in enumerate(pieces[piece]):
            at = i if piece == 0 else piece + 2
            made.append(pltpu.make_async_remote_copy(
                src_ref=part(entry, slot_from), dst_ref=part(entry, slot_to),
                send_sem=send.at[where, at], recv_sem=recv.at[slot_to - 1, at],
                device_id={"blk": target[0], "batch": target[1]},
            ))
        return made

    def start(copies):
        for c in copies:
            c.start()

    def first_hop(piece):
        return hop(0, 2, piece, 1, bl_send, bl_recv, (after, bat))

    def to_odd(piece):
        return hop(0, 1, piece, 0, bl_send, bl_recv, (pair, bat))

    def odd_forward(piece):
        return hop(2, 1, piece, 0, bl_send, bl_recv, (pair, bat))

    def even_forward(piece):
        return hop(2, 3, piece, 2, bl_send, bl_recv, (pair, bat))

    def even_onward(piece):
        return hop(1, 3, piece, 3, bl_send, bl_recv, (after, bat))

    def share(slot, piece):
        return hop(slot, slot, piece, slot - 1, fw_send, fw_recv, (blk, sibling))

    def take(slot, piece):
        for c in hop(slot, slot, piece, slot - 1, bl_send, bl_recv, (pair, bat)):
            c.wait_recv()
        if slot == 2:
            @pl.when(odd == 0)
            def _():
                start(even_forward(piece))

            @pl.when(odd == 1)
            def _():
                start(odd_forward(piece))
        if slot == 1:
            @pl.when(odd == 0)
            def _():
                start(even_onward(piece))
        start(share(slot, piece))

    def shared(slot):
        for p in range(count):
            for c in share(slot, p):
                c.wait_recv()

    moves = [[] for _ in range(chunks)]
    for c in range(chunks):
        for i, q in enumerate(partners):
            moves[c].append(pltpu.make_async_remote_copy(
                src_ref=stage.at[:, :, rows_of(q, c)],
                dst_ref=trv.at[bat, :, :, pl.ds(c * ROWS, ROWS)],
                send_sem=tr_send.at[c, i], recv_sem=tr_recv.at[c, i],
                device_id={"blk": blk, "batch": q},
            ))

    pl.semaphore_wait(barrier, len(partners) + 3)
    own[0].wait()
    start(moves[0])
    for c in own[1:4]:
        c.wait()
    for p in range(count):
        start(first_hop(p))

    @pl.when(odd == 0)
    def _():
        for p in range(count):
            start(to_odd(p))

    for c in range(1, chunks):
        start(moves[c])

    place_weights(wes.at[0], n_batch, wv.at[0])
    own[4].wait()
    rest = jnp.zeros((LANES - k, ROWS), F32)
    for c in range(chunks):
        block = jnp.concatenate([cov[:, c * ROWS:(c + 1) * ROWS].astype(F32), rest], axis=0)
        co_t[c] = block.T.astype(BF16)
    own[5].wait()

    gap = jnp.zeros((SLOT - jl, ROWS), F32)

    def turn(c):
        for d in range(3):
            parts = []
            for q in range(4):
                for i in range(n_batch):
                    parts += [trv[i, 4 * d + q, :, c * ROWS:(c + 1) * ROWS].astype(F32), gap]
            po_t[d, c] = jnp.concatenate(parts, axis=0).T.astype(BF16)

    def unit(step, c):
        def put(d, at, value):
            mix[d, c, pl.ds(at, ROWS, stride=PITCH), :] = value
        skin_rows(
            step, co_t.at[c], [po_t[d, c] for d in range(3)], bas.at[step], tes.at[step], wv.at[step], put
        )

    def early(c):
        for i in range(n_batch - 1):
            moves[c][i].wait_recv()
        turn(c)
        unit(0, c)

    early(0)
    early(1)
    take(2, 0)
    early(2)
    take(2, 1)
    early(3)
    take(2, 2)
    early(4)
    take(1, 0)
    early(5)

    shared(2)
    place_weights(wes.at[2], n_batch, wv.at[2])
    group = 2

    def sweep(step, polls):
        for b in range(chunks // group):
            for c in range(group):
                unit(step, b * group + c)
            if b < len(polls):
                take(*polls[b])

    sweep(2, [(1, 1), (1, 2)])
    shared(1)
    place_weights(wes.at[1], n_batch, wv.at[1])
    sweep(1, [(3, 0), (3, 1)])
    take(3, 2)
    shared(3)

    for c in range(chunks):
        for m in moves[c]:
            m.wait_send()
    for p in range(count):
        for slot in (2, 1, 3):
            for c in share(slot, p):
                c.wait_send()
        for c in first_hop(p) + to_odd(p):
            c.wait_send()

        @pl.when(odd == 0)
        def _():
            for c in even_forward(p) + even_onward(p):
                c.wait_send()


def front(n_blk, n_batch, coefficients, transforms, basis, template, weights):
    comps, jl, total = transforms.shape
    chars = total // n_batch
    chunks = chars // ROWS
    k = coefficients.shape[0]
    verts = weights.shape[1]
    joints = weights.shape[0]
    hop = STEPS - 1
    assert n_blk % 2 == 0 and n_blk > STEPS and n_batch % 2 == 0 and STEPS == 4
    assert chars % ROWS == 0 and k <= LANES and comps == 12
    assert joints == n_batch * jl and jl <= SLOT and 4 * n_batch * SLOT == LANES
    dma = pltpu.SemaphoreType.DMA
    any_spec = pl.BlockSpec(memory_space=pl.ANY)
    vmem_spec = pl.BlockSpec(memory_space=pltpu.VMEM)
    inputs = [
        pltpu.with_memory_space_constraint(a, pltpu.HBM)
        for a in (coefficients, transforms, basis, template, weights)
    ]
    return pl.pallas_call(
        functools.partial(front_kernel, n_blk, n_batch),
        out_shape=(
            pltpu.VMEM((3, chunks, ROWS * PITCH, LANES), F32),
            pltpu.VMEM((chunks, ROWS, LANES), BF16),
            pltpu.VMEM((3, chunks, ROWS, LANES), BF16),
            pltpu.VMEM((STEPS,) + basis.shape, BF16),
            pltpu.VMEM((STEPS,) + template.shape, BF16),
            pltpu.VMEM((STEPS,) + weights.shape, BF16),
        ),
        in_specs=[any_spec] * 5,
        out_specs=(vmem_spec,) * 6,
        scratch_shapes=[
            pltpu.VMEM((k, chars), BF16),
            pltpu.VMEM(transforms.shape, BF16),
            pltpu.VMEM((n_batch, comps, jl, chars), BF16),
            pltpu.VMEM((hop, 4, LANES, verts), BF16),
            dma((chunks, n_batch - 1)), dma((chunks, n_batch - 1)),
            dma((hop + 1, 5)), dma((hop, 5)), dma((hop, 5)), dma((hop, 5)), dma((6,)),
        ],
        compiler_params=pltpu.CompilerParams(
            collective_id=0, has_side_effects=True, vmem_limit_bytes=16 << 20
        ),
        cost_estimate=pl.CostEstimate(flops=0, bytes_accessed=20 << 20, transcendentals=0),
        name="front",
    )(*inputs)


def back_kernel(
    n_batch, mix_in, co_t, po_t, bas, tes, wes, out_ref, mix, wv, staged, sem,
):
    chunks = co_t.shape[0]
    wv[...] = jnp.zeros_like(wv)
    place_weights(wes.at[LAST], n_batch, wv)

    def send(c):
        return pltpu.make_async_copy(
            staged.at[lax.rem(c, 2)], out_ref.at[pl.ds(c * ROWS, ROWS)], sem.at[lax.rem(c, 2)]
        )

    for c in range(chunks):
        def put(d, at, value):
            mix[d, c, pl.ds(at, ROWS, stride=PITCH), :] = value
        skin_rows(
            LAST, co_t.at[c], [po_t[d, c] for d in range(3)], bas.at[LAST], tes.at[LAST], wv, put
        )
        if c >= 2:
            send(c - 2).wait()
        for r in range(ROWS):
            for d in range(3):
                low = mix[d, c, pl.ds(r * PITCH, 8, stride=2), :]
                high = mix[d, c, pl.ds(r * PITCH + 1, 8, stride=2), :]
                staged[c % 2, r, d] = jnp.concatenate([low, high], axis=0).astype(BF16)
        send(c).start()
    for c in range(max(chunks - 2, 0), chunks):
        send(c).wait()


def back(n_batch, mix, co_t, po_t, bas, tes, wes):
    chunks = co_t.shape[0]
    chars = chunks * ROWS
    verts = wes.shape[2]
    group = (verts // LANES) * STEPS
    any_spec = pl.BlockSpec(memory_space=pl.ANY)
    vmem_spec = pl.BlockSpec(memory_space=pltpu.VMEM)
    out, _ = pl.pallas_call(
        functools.partial(back_kernel, n_batch),
        out_shape=(
            jax.ShapeDtypeStruct((chars, 3, group, LANES), BF16),
            pltpu.VMEM(mix.shape, F32),
        ),
        in_specs=[vmem_spec] * 6,
        out_specs=(any_spec, vmem_spec),
        input_output_aliases={0: 1},
        scratch_shapes=[
            pltpu.VMEM((4, LANES, verts), BF16),
            pltpu.VMEM((2, ROWS, 3, group, LANES), BF16),
            pltpu.SemaphoreType.DMA((2,)),
        ],
        compiler_params=pltpu.CompilerParams(vmem_limit_bytes=16 << 20),
        name="back",
    )(mix, co_t, po_t, bas, tes, wes)
    out = out.reshape(chars, 3, verts // LANES, STEPS, LANES)
    return out.transpose(0, 3, 1, 2, 4).reshape(chars, STEPS, 3, verts)


def solution(mesh):
    n_blk, n_batch = mesh.shape["blk"], mesh.shape["batch"]

    def per_device(coefficients, transforms, basis, template, skin_weights):
        basis = jnp.transpose(basis, (1, 0, 2))
        return back(n_batch, *front(
            n_blk, n_batch, coefficients, transforms, basis, template, skin_weights
        ))

    in_specs = (
        P(None, ("blk", "batch")),
        P(None, "batch", "blk"),
        P(None, None, "blk"),
        P(None, "blk"),
        P(None, "blk"),
    )
    out_specs = P(("blk", "batch"), None, None, None)
    return jax.shard_map(
        per_device, mesh=mesh, in_specs=in_specs, out_specs=out_specs, check_vma=False
    )
```

```python
import functools
import jax
import jax.numpy as jnp
from jax import lax
from jax.experimental import pallas as pl
from jax.experimental.pallas import tpu as pltpu
from jax.sharding import PartitionSpec as P

STEPS = 4
LANES = 128
WIDE = 256
ROWS = 128
PITCH = 20
PARTS = 2
CUT = 64
BF16 = jnp.bfloat16
F32 = jnp.float32
LAST = STEPS - 1


def place_weights(raw, n_batch, wv):
    joints, verts = raw.shape
    jl = joints // n_batch
    w = raw[...].astype(F32)
    w = (w / jnp.sum(w, axis=0, keepdims=True)).astype(BF16).astype(F32)
    for q in range(4):
        parts = []
        for i in range(n_batch):
            if q > 0:
                parts.append(jnp.zeros((q * jl, verts), F32))
            parts.append(w[i * jl:(i + 1) * jl])
            if q < 3:
                parts.append(jnp.zeros(((3 - q) * jl, verts), F32))
        if 4 * joints < LANES:
            parts.append(jnp.zeros((LANES - 4 * joints, verts), F32))
        wv[q] = jnp.concatenate(parts, axis=0).astype(BF16)


def shape_rows(coefs, basis, te, n):
    k = basis.shape[1]
    cols = slice(n * WIDE, (n + 1) * WIDE)
    return [
        jnp.dot(coefs[:, :k], basis[e, :, cols], preferred_element_type=F32) + te[e:e + 1, cols].astype(F32)
        for e in range(3)
    ]


def skin_rows(step, shaped_of, poses, wv, put):
    verts = wv.shape[2]
    for n in range(verts // WIDE):
        cols = slice(n * WIDE, (n + 1) * WIDE)
        shaped = shaped_of(n)
        for d in range(3):
            total = jnp.dot(poses[d], wv[3, :, cols], preferred_element_type=F32)
            for e in range(3):
                total = total + shaped[e] * jnp.dot(poses[d], wv[e, :, cols], preferred_element_type=F32)
            for h in range(WIDE // LANES):
                t = n * (WIDE // LANES) + h
                put(d, 8 * (t % 2) + t // 2 + 2 * step, total[:, h * LANES:(h + 1) * LANES])


WHEN = {
    "even": {2: (0, 1, 2, 3, 4, 5), 1: (4, 5, 6, 8, 8, 10), 3: (16, 16, 16, 18, 18, 18)},
    "odd": {2: (0, 1, 2, 3, 4, 5), 1: (1, 2, 3, 4, 5, 5), 3: (8, 8, 10, 10, 12, 12)},
    "even wrap": {2: (4, 5, 5, 6, 6, 6), 1: (8, 8, 8, 10, 11, 11), 3: (14, 14, 16, 16, 18, 18)},
    "odd wrap": {2: (3, 4, 5, 6, 6, 6), 1: (1, 2, 3, 4, 5, 5), 3: (14, 14, 16, 16, 18, 18)},
}


def takes_before(at, chunks, count):
    found = {}
    for kind, slots in WHEN.items():
        for slot, times in slots.items():
            for p in range(count):
                if times[p * 6 // count] * chunks // 6 == at:
                    found.setdefault((slot, p), []).append(kind)
    return sorted(found.items(), key=lambda item: ((2, 1, 3).index(item[0][0]), item[0][1]))


def front_kernel(
    n_blk, n_batch, co_ref, tr_ref, ba_ref, te_ref, we_ref,
    mix, co_t, po_t, bas, tes, wv_last,
    cov, stage, packed, trv, wes, wv, early_shape,
    tr_send, tr_recv, bl_send, bl_recv, fw_send, fw_recv, own_sem,
):
    blk, bat = lax.axis_index("blk"), lax.axis_index("batch")
    sibling = bat + 1 - 2 * lax.rem(bat, 2)
    odd = lax.rem(blk, 2)
    pair = blk + 1 - 2 * odd
    after = lax.rem(blk + 2, n_blk)
    before = lax.rem(blk + n_blk - 2, n_blk)
    chars = trv.shape[3]
    chunks = chars // ROWS
    jl = stage.shape[1]
    k = cov.shape[0]
    verts = bas.shape[3]
    half = verts // 2

    own = [
        pltpu.make_async_copy(we_ref, wes.at[0], own_sem.at[0]),
        pltpu.make_async_copy(te_ref, tes.at[0], own_sem.at[1]),
        pltpu.make_async_copy(ba_ref, bas.at[0], own_sem.at[2]),
        pltpu.make_async_copy(tr_ref, stage, own_sem.at[3]),
        pltpu.make_async_copy(co_ref, cov, own_sem.at[4]),
    ]

    partners = [lax.rem(bat + i, n_batch) for i in range(1, n_batch)]
    barrier = pltpu.get_barrier_semaphore()
    for q in partners:
        pl.semaphore_signal(barrier, inc=1, device_id={"blk": blk, "batch": q})
    for b in (pair, before):
        pl.semaphore_signal(barrier, inc=1, device_id={"blk": b, "batch": bat})
    for c in own:
        c.start()

    mine = pl.ds(pl.multiple_of(lax.rem(bat, 2) * half, LANES), half)
    pieces = []
    for e in range(3):
        for low in range(0, k, CUT):
            pieces.append([(bas, e, pl.ds(low, min(CUT, k - low)))])
    pieces[0] = [tes, wes] + pieces[0]
    count = len(pieces)

    def part(entry, slot):
        if isinstance(entry, tuple):
            return entry[0].at[slot, entry[1], entry[2], mine]
        return entry.at[slot, :, mine]

    def kind_of(piece, i):
        return i if piece == 0 else 2

    def hop(slot_from, slot_to, piece, where, send, recv, target, shared=False):
        made = []
        for i, entry in enumerate(pieces[piece]):
            kind = kind_of(piece, i)
            at = kind if shared or kind < 2 else piece + 2
            made.append(pltpu.make_async_remote_copy(
                src_ref=part(entry, slot_from), dst_ref=part(entry, slot_to),
                send_sem=send.at[where, kind], recv_sem=recv.at[slot_to - 1, at],
                device_id={"blk": target[0], "batch": target[1]},
            ))
        return made

    def all_pieces(where, send, recv, slot):
        return [
            pltpu.make_async_remote_copy(
                src_ref=ref, dst_ref=ref, send_sem=send.at[where, kind], recv_sem=recv.at[slot - 1, kind],
                device_id={"blk": blk, "batch": sibling},
            )
            for kind, ref in enumerate(
                (tes.at[slot, :, mine], wes.at[slot, :, mine], bas.at[slot, :, :, mine])
            )
        ]

    def start(copies):
        for c in copies:
            c.start()

    def first_hop(piece):
        return hop(0, 2, piece, 1, bl_send, bl_recv, (after, bat))

    def to_odd(piece):
        return hop(0, 1, piece, 0, bl_send, bl_recv, (pair, bat))

    def across(piece):
        return hop(2, 3 - 2 * odd, piece, 2, bl_send, bl_recv, (pair, bat))

    def onward(piece):
        return hop(1, 3, piece, 3, bl_send, bl_recv, (after, bat))

    def share(slot, piece):
        return hop(slot, slot, piece, slot - 1, fw_send, fw_recv, (blk, sibling), shared=True)

    wrap = blk < 2
    is_kind = {
        "even": jnp.logical_and(odd == 0, jnp.logical_not(wrap)),
        "odd": jnp.logical_and(odd == 1, jnp.logical_not(wrap)),
        "even wrap": jnp.logical_and(odd == 0, wrap),
        "odd wrap": jnp.logical_and(odd == 1, wrap),
    }

    def take(slot, piece, kinds):
        def body():
            for c in hop(slot, slot, piece, slot - 1, bl_send, bl_recv, (pair, bat)):
                c.wait_recv()
            if slot == 2:
                start(across(piece))
            if slot == 1:
                @pl.when(odd == 0)
                def _():
                    start(onward(piece))
            start(share(slot, piece))

        if len(kinds) == len(is_kind):
            body()
        else:
            pl.when(functools.reduce(jnp.logical_or, [is_kind[x] for x in kinds]))(body)

    def got(slot, kinds):
        copies = all_pieces(slot - 1, fw_send, fw_recv, slot)
        for kind in kinds:
            copies[kind].wait_recv()

    moves = [[] for _ in range(chunks)]
    for c in range(chunks):
        for i, q in enumerate(partners):
            moves[c].append(pltpu.make_async_remote_copy(
                src_ref=packed.at[i, :, :, pl.ds(c * ROWS, ROWS)],
                dst_ref=trv.at[bat, :, :, pl.ds(c * ROWS, ROWS)],
                send_sem=tr_send.at[i], recv_sem=tr_recv.at[c],
                device_id={"blk": blk, "batch": q},
            ))

    def wide_move(i, count, cols):
        ref = trv.at[pl.ds(0, count), :, :, cols]
        return pltpu.make_async_remote_copy(
            src_ref=ref, dst_ref=ref, send_sem=tr_send.at[i], recv_sem=tr_recv.at[cols.start // ROWS],
            device_id={"blk": blk, "batch": partners[i]},
        )


    for c in own[:3]:
        c.wait()
    pl.semaphore_wait(barrier, len(partners) + 2)
    for p in range(count):
        start(first_hop(p))

    @pl.when(odd == 0)
    def _():
        for p in range(count):
            start(to_odd(p))

    own[3].wait()
    for i, q in enumerate(partners + [bat]):
        for c in range(chunks):
            cols = pl.ds(pl.multiple_of(q * chars + c * ROWS, LANES), ROWS)
            for d in range(3):
                rows = jnp.concatenate(
                    [stage[4 * d + e, :, cols].astype(F32) for e in range(4)], axis=0
                ).astype(BF16)
                if i < n_batch - 1:
                    packed[i, d, :, c * ROWS:(c + 1) * ROWS] = rows
                else:
                    trv[bat, d, :, c * ROWS:(c + 1) * ROWS] = rows

    for c in range(chunks):
        start(moves[c])

    place_weights(wes.at[0], n_batch, wv.at[0])
    own[4].wait()
    rest = jnp.zeros((LANES - k, ROWS), F32)
    for c in range(chunks):
        block = jnp.concatenate([cov[:, c * ROWS:(c + 1) * ROWS].astype(F32), rest], axis=0)
        co_t[c] = block.T.astype(BF16)
    for c in range(chunks):
        for n in range(verts // WIDE):
            for e, value in enumerate(shape_rows(co_t[c], bas.at[0], tes.at[0], n)):
                early_shape[c, n, e] = value

    def turn(c):
        for d in range(3):
            parts = [trv[i, d, :, c * ROWS:(c + 1) * ROWS].astype(F32) for i in range(n_batch)]
            if 4 * n_batch * jl < LANES:
                parts.append(jnp.zeros((LANES - 4 * n_batch * jl, ROWS), F32))
            po_t[d, c] = jnp.concatenate(parts, axis=0).T.astype(BF16)

    def unit(step, c, shaped_of=None):
        def put(d, at, value):
            mix[d, c, pl.ds(at, ROWS, stride=PITCH), :] = value

        def fresh(n):
            return shape_rows(co_t[c], bas.at[step], tes.at[step], n)

        skin_rows(step, shaped_of or fresh, [po_t[d, c] for d in range(3)], wv.at[step], put)

    def early(c):
        wide_move(0, n_batch - 1, slice(c * ROWS, (c + 1) * ROWS)).wait_recv()
        turn(c)
        unit(0, c, lambda n: [early_shape[c, n, e] for e in range(3)])

    order = (2 - odd, 1 + odd)
    for at in range(3 * chunks + 1):
        for (slot, piece), kinds in takes_before(at, chunks, count):
            take(slot, piece, kinds)
        turn_of, c = at // chunks, at % chunks
        if turn_of < 2 and c == chunks - 1:
            got(order[turn_of], (0, 1))
            place_weights(wes.at[order[turn_of]], n_batch, wv.at[order[turn_of]])
        if turn_of == 2 and c == chunks - 1:
            got(LAST, (0, 1))
            place_weights(wes.at[LAST], n_batch, wv_last)
        if turn_of == 0:
            early(c)
        if turn_of > 0 and c == 0:
            got(order[turn_of - 1] if turn_of < 3 else LAST, (2,))
        if 0 < turn_of < 3:
            unit(order[turn_of - 1], c)

    for i in range(n_batch - 1):
        wide_move(i, 1, slice(0, chars)).wait_send()
    for slot in (2, 1, 3):
        for c in all_pieces(slot - 1, fw_send, fw_recv, slot):
            c.wait_send()
    for where in (1, 2):
        for c in all_pieces(where, bl_send, bl_recv, 1):
            c.wait_send()

    @pl.when(odd == 0)
    def _():
        for where in (0, 3):
            for c in all_pieces(where, bl_send, bl_recv, 1):
                c.wait_send()


def front(n_blk, n_batch, coefficients, transforms, basis, template, weights):
    comps, jl, total = transforms.shape
    chars = total // n_batch
    chunks = chars // ROWS
    k = coefficients.shape[0]
    verts = weights.shape[1]
    joints = weights.shape[0]
    hop = STEPS - 1
    assert n_blk % 2 == 0 and n_blk > STEPS and n_batch % 2 == 0 and STEPS == 4
    assert chars % ROWS == 0 and k <= LANES and comps == 12
    assert joints == n_batch * jl and 4 * joints <= LANES
    sems = 3 * -(-k // CUT) + 2
    dma = pltpu.SemaphoreType.DMA
    any_spec = pl.BlockSpec(memory_space=pl.ANY)
    vmem_spec = pl.BlockSpec(memory_space=pltpu.VMEM)
    inputs = [
        pltpu.with_memory_space_constraint(a, pltpu.HBM)
        for a in (coefficients, transforms, basis, template, weights)
    ]
    return pl.pallas_call(
        functools.partial(front_kernel, n_blk, n_batch),
        out_shape=(
            pltpu.VMEM((3, chunks, ROWS * PITCH, LANES), F32),
            pltpu.VMEM((chunks, ROWS, LANES), BF16),
            pltpu.VMEM((3, chunks, ROWS, LANES), BF16),
            pltpu.VMEM((STEPS,) + basis.shape, BF16),
            pltpu.VMEM((STEPS,) + template.shape, BF16),
            pltpu.VMEM((4, LANES, verts), BF16),
        ),
        in_specs=[any_spec] * 5,
        out_specs=(vmem_spec,) * 6,
        scratch_shapes=[
            pltpu.VMEM((k, chars), BF16),
            pltpu.VMEM(transforms.shape, BF16),
            pltpu.VMEM((n_batch - 1, 3, 4 * jl, chars), BF16),
            pltpu.VMEM((n_batch, 3, 4 * jl, chars), BF16),
            pltpu.VMEM((STEPS,) + weights.shape, BF16),
            pltpu.VMEM((hop, 4, LANES, verts), BF16),
            pltpu.VMEM((chunks, verts // WIDE, 3, ROWS, WIDE), F32),
            dma((n_batch - 1,)), dma((chunks,)),
            dma((hop + 1, 3)), dma((hop, sems)), dma((hop, 3)), dma((hop, 3)), dma((5,)),
        ],
        compiler_params=pltpu.CompilerParams(
            collective_id=0, has_side_effects=True, vmem_limit_bytes=20 << 20
        ),
        cost_estimate=pl.CostEstimate(flops=0, bytes_accessed=20 << 20, transcendentals=0),
        name="front",
    )(*inputs)


def back_kernel(mix_in, co_t, po_t, bas, tes, wv, out_ref, mix, staged, sem):
    chunks = co_t.shape[0]
    part = ROWS // PARTS

    def send(c, p):
        return pltpu.make_async_copy(
            staged.at[c, pl.ds(p * part, part)], out_ref.at[pl.ds(c * ROWS + p * part, part)], sem.at[c, p]
        )

    def pack(c, p):
        for r in range(p * part, (p + 1) * part):
            for d in range(3):
                low = mix[d, c, pl.ds(r * PITCH, 8, stride=2), :]
                high = mix[d, c, pl.ds(r * PITCH + 1, 8, stride=2), :]
                staged[c, r, d] = jnp.concatenate([low, high], axis=0).astype(BF16)

    for c in range(chunks):
        def put(d, at, value):
            mix[d, c, pl.ds(at, ROWS, stride=PITCH), :] = value

        skin_rows(
            LAST, lambda n: shape_rows(co_t[c], bas.at[LAST], tes.at[LAST], n),
            [po_t[d, c] for d in range(3)], wv, put,
        )
        if c > 0:
            for p in range(PARTS):
                pack(c - 1, p)
            for p in range(PARTS):
                send(c - 1, p).start()
    for p in range(PARTS):
        pack(chunks - 1, p)
        send(chunks - 1, p).start()
    for c in range(chunks):
        for p in range(PARTS):
            send(c, p).wait()


def back(mix, co_t, po_t, bas, tes, wv):
    chunks = co_t.shape[0]
    chars = chunks * ROWS
    verts = wv.shape[2]
    group = (verts // LANES) * STEPS
    any_spec = pl.BlockSpec(memory_space=pl.ANY)
    vmem_spec = pl.BlockSpec(memory_space=pltpu.VMEM)
    out, _ = pl.pallas_call(
        back_kernel,
        out_shape=(
            jax.ShapeDtypeStruct((chars, 3, group, LANES), BF16),
            pltpu.VMEM(mix.shape, F32),
        ),
        in_specs=[vmem_spec] * 6,
        out_specs=(any_spec, vmem_spec),
        input_output_aliases={0: 1},
        scratch_shapes=[
            pltpu.VMEM((chunks, ROWS, 3, group, LANES), BF16),
            pltpu.SemaphoreType.DMA((chunks, PARTS)),
        ],
        compiler_params=pltpu.CompilerParams(vmem_limit_bytes=20 << 20),
        name="back",
    )(mix, co_t, po_t, bas, tes, wv)
    out = out.reshape(chars, 3, verts // LANES, STEPS, LANES)
    return out.transpose(0, 3, 1, 2, 4).reshape(chars, STEPS, 3, verts)


def solution(mesh):
    n_blk, n_batch = mesh.shape["blk"], mesh.shape["batch"]

    def per_device(coefficients, transforms, basis, template, skin_weights):
        basis = jnp.transpose(basis, (1, 0, 2))
        return back(*front(
            n_blk, n_batch, coefficients, transforms, basis, template, skin_weights
        ))

    in_specs = (
        P(None, ("blk", "batch")),
        P(None, "batch", "blk"),
        P(None, None, "blk"),
        P(None, "blk"),
        P(None, "blk"),
    )
    out_specs = P(("blk", "batch"), None, None, None)
    return jax.shard_map(
        per_device, mesh=mesh, in_specs=in_specs, out_specs=out_specs, check_vma=False
    )
```

```python
import functools
import jax
import jax.numpy as jnp
from jax import lax
from jax.experimental import pallas as pl
from jax.experimental.pallas import tpu as pltpu
from jax.sharding import PartitionSpec as P

STEPS = 4
LANES = 128
WIDE = 256
ROWS = 128
PITCH = 20
PARTS = 4
CUT = 64
BF16 = jnp.bfloat16
F32 = jnp.float32
LAST = STEPS - 1


def place_weights(raw, n_batch, wv):
    joints, verts = raw.shape
    jl = joints // n_batch
    w = raw[...].astype(F32)
    w = (w / jnp.sum(w, axis=0, keepdims=True)).astype(BF16).astype(F32)
    for q in range(4):
        parts = []
        for i in range(n_batch):
            if q > 0:
                parts.append(jnp.zeros((q * jl, verts), F32))
            parts.append(w[i * jl:(i + 1) * jl])
            if q < 3:
                parts.append(jnp.zeros(((3 - q) * jl, verts), F32))
        if 4 * joints < LANES:
            parts.append(jnp.zeros((LANES - 4 * joints, verts), F32))
        wv[q] = jnp.concatenate(parts, axis=0).astype(BF16)


def shape_rows(coefs, basis, te, n):
    k = basis.shape[1]
    cols = slice(n * WIDE, (n + 1) * WIDE)
    return [
        jnp.dot(coefs[:, :k], basis[e, :, cols], preferred_element_type=F32) + te[e:e + 1, cols].astype(F32)
        for e in range(3)
    ]


def skin_rows(step, shaped_of, poses, wv, put):
    verts = wv.shape[2]
    for n in range(verts // WIDE):
        cols = slice(n * WIDE, (n + 1) * WIDE)
        shaped = shaped_of(n)
        for d in range(3):
            total = jnp.dot(poses[d], wv[3, :, cols], preferred_element_type=F32)
            for e in range(3):
                total = total + shaped[e] * jnp.dot(poses[d], wv[e, :, cols], preferred_element_type=F32)
            for h in range(WIDE // LANES):
                t = n * (WIDE // LANES) + h
                put(d, 8 * (t % 2) + t // 2 + 2 * step, total[:, h * LANES:(h + 1) * LANES])


WHEN = {
    "even": {2: (0, 1, 2, 3, 4, 5), 1: (3, 4, 5, 6, 8, 8), 3: (12, 16, 16, 16, 16, 16)},
    "odd": {2: (0, 1, 1, 2, 3, 4), 1: (1, 2, 3, 4, 5, 5), 3: (8, 8, 10, 10, 12, 12)},
    "even wrap": {2: (4, 5, 5, 6, 6, 6), 1: (8, 8, 10, 10, 11, 11), 3: (12, 16, 16, 16, 16, 16)},
    "odd wrap": {2: (3, 4, 5, 6, 6, 6), 1: (1, 2, 3, 4, 5, 5), 3: (12, 16, 16, 16, 16, 16)},
}


def takes_before(at, chunks, count):
    found = {}
    for kind, slots in WHEN.items():
        for slot, times in slots.items():
            for p in range(count):
                if times[p * 6 // count] * chunks // 6 == at:
                    found.setdefault((slot, p), []).append(kind)
    return sorted(found.items(), key=lambda item: ((2, 1, 3).index(item[0][0]), item[0][1]))


def front_kernel(
    n_blk, n_batch, co_ref, tr_ref, ba_ref, te_ref, we_ref,
    mix, co_t, po_t, bas, tes, wv_last,
    cov, stage, packed, trv, wes, wv, early_shape,
    tr_send, tr_recv, bl_send, bl_recv, fw_send, fw_recv, own_sem,
):
    blk, bat = lax.axis_index("blk"), lax.axis_index("batch")
    sibling = bat + 1 - 2 * lax.rem(bat, 2)
    odd = lax.rem(blk, 2)
    pair = blk + 1 - 2 * odd
    after = lax.rem(blk + 2, n_blk)
    before = lax.rem(blk + n_blk - 2, n_blk)
    chars = trv.shape[3]
    chunks = chars // ROWS
    jl = stage.shape[1]
    k = cov.shape[0]
    verts = bas.shape[3]
    half = verts // 2

    own = [
        pltpu.make_async_copy(we_ref, wes.at[0], own_sem.at[0]),
        pltpu.make_async_copy(te_ref, tes.at[0], own_sem.at[1]),
        pltpu.make_async_copy(ba_ref, bas.at[0], own_sem.at[2]),
        pltpu.make_async_copy(tr_ref, stage, own_sem.at[3]),
        pltpu.make_async_copy(co_ref, cov, own_sem.at[4]),
    ]

    partners = [lax.rem(bat + i, n_batch) for i in range(1, n_batch)]
    barrier = pltpu.get_barrier_semaphore()
    for q in partners:
        pl.semaphore_signal(barrier, inc=1, device_id={"blk": blk, "batch": q})
    for b in (pair, before):
        pl.semaphore_signal(barrier, inc=1, device_id={"blk": b, "batch": bat})
    for c in own:
        c.start()

    mine = pl.ds(pl.multiple_of(lax.rem(bat, 2) * half, LANES), half)
    pieces = []
    for e in range(3):
        for low in range(0, k, CUT):
            pieces.append([(bas, e, pl.ds(low, min(CUT, k - low)))])
    pieces[0] = [tes, wes] + pieces[0]
    count = len(pieces)

    def part(entry, slot):
        if isinstance(entry, tuple):
            return entry[0].at[slot, entry[1], entry[2], mine]
        return entry.at[slot, :, mine]

    def kind_of(piece, i):
        return i if piece == 0 else 2

    def hop(slot_from, slot_to, piece, where, send, recv, target, shared=False):
        made = []
        for i, entry in enumerate(pieces[piece]):
            kind = kind_of(piece, i)
            at = kind if shared or kind < 2 else piece + 2
            made.append(pltpu.make_async_remote_copy(
                src_ref=part(entry, slot_from), dst_ref=part(entry, slot_to),
                send_sem=send.at[where, kind], recv_sem=recv.at[slot_to - 1, at],
                device_id={"blk": target[0], "batch": target[1]},
            ))
        return made

    def all_pieces(where, send, recv, slot):
        return [
            pltpu.make_async_remote_copy(
                src_ref=ref, dst_ref=ref, send_sem=send.at[where, kind], recv_sem=recv.at[slot - 1, kind],
                device_id={"blk": blk, "batch": sibling},
            )
            for kind, ref in enumerate(
                (tes.at[slot, :, mine], wes.at[slot, :, mine], bas.at[slot, :, :, mine])
            )
        ]

    def start(copies):
        for c in copies:
            c.start()

    def first_hop(piece):
        return hop(0, 2, piece, 1, bl_send, bl_recv, (after, bat))

    def to_odd(piece):
        return hop(0, 1, piece, 0, bl_send, bl_recv, (pair, bat))

    def across(piece):
        return hop(2, 3 - 2 * odd, piece, 2, bl_send, bl_recv, (pair, bat))

    def onward(piece):
        return hop(1, 3, piece, 3, bl_send, bl_recv, (after, bat))

    def share(slot, piece):
        return hop(slot, slot, piece, slot - 1, fw_send, fw_recv, (blk, sibling), shared=True)

    wrap = blk < 2
    is_kind = {
        "even": jnp.logical_and(odd == 0, jnp.logical_not(wrap)),
        "odd": jnp.logical_and(odd == 1, jnp.logical_not(wrap)),
        "even wrap": jnp.logical_and(odd == 0, wrap),
        "odd wrap": jnp.logical_and(odd == 1, wrap),
    }

    def take(slot, piece, kinds):
        def body():
            for c in hop(slot, slot, piece, slot - 1, bl_send, bl_recv, (pair, bat)):
                c.wait_recv()
            if slot == 2:
                start(across(piece))
            if slot == 1:
                @pl.when(odd == 0)
                def _():
                    start(onward(piece))
            start(share(slot, piece))

        if len(kinds) == len(is_kind):
            body()
        else:
            pl.when(functools.reduce(jnp.logical_or, [is_kind[x] for x in kinds]))(body)

    def got(slot, kinds):
        copies = all_pieces(slot - 1, fw_send, fw_recv, slot)
        for kind in kinds:
            copies[kind].wait_recv()

    moves = [[] for _ in range(chunks)]
    for c in range(chunks):
        for i, q in enumerate(partners):
            moves[c].append(pltpu.make_async_remote_copy(
                src_ref=packed.at[i, :, :, pl.ds(c * ROWS, ROWS)],
                dst_ref=trv.at[bat, :, :, pl.ds(c * ROWS, ROWS)],
                send_sem=tr_send.at[i], recv_sem=tr_recv.at[c],
                device_id={"blk": blk, "batch": q},
            ))

    def wide_move(i, count, cols):
        ref = trv.at[pl.ds(0, count), :, :, cols]
        return pltpu.make_async_remote_copy(
            src_ref=ref, dst_ref=ref, send_sem=tr_send.at[i], recv_sem=tr_recv.at[cols.start // ROWS],
            device_id={"blk": blk, "batch": partners[i]},
        )


    for c in own[:3]:
        c.wait()
    pl.semaphore_wait(barrier, len(partners) + 2)
    for p in range(count):
        start(first_hop(p))

    @pl.when(odd == 0)
    def _():
        for p in range(count):
            start(to_odd(p))

    own[3].wait()
    for i, q in enumerate(partners + [bat]):
        for c in range(chunks):
            cols = pl.ds(pl.multiple_of(q * chars + c * ROWS, LANES), ROWS)
            for d in range(3):
                rows = jnp.concatenate(
                    [stage[4 * d + e, :, cols].astype(F32) for e in range(4)], axis=0
                ).astype(BF16)
                if i < n_batch - 1:
                    packed[i, d, :, c * ROWS:(c + 1) * ROWS] = rows
                else:
                    trv[bat, d, :, c * ROWS:(c + 1) * ROWS] = rows

    for c in range(chunks):
        start(moves[c])

    place_weights(wes.at[0], n_batch, wv.at[0])
    own[4].wait()
    rest = jnp.zeros((LANES - k, ROWS), F32)
    for c in range(chunks):
        block = jnp.concatenate([cov[:, c * ROWS:(c + 1) * ROWS].astype(F32), rest], axis=0)
        co_t[c] = block.T.astype(BF16)
    for c in range(chunks):
        for n in range(verts // WIDE):
            for e, value in enumerate(shape_rows(co_t[c], bas.at[0], tes.at[0], n)):
                early_shape[c, n, e] = value

    def turn(c):
        for d in range(3):
            parts = [trv[i, d, :, c * ROWS:(c + 1) * ROWS].astype(F32) for i in range(n_batch)]
            if 4 * n_batch * jl < LANES:
                parts.append(jnp.zeros((LANES - 4 * n_batch * jl, ROWS), F32))
            po_t[d, c] = jnp.concatenate(parts, axis=0).T.astype(BF16)

    def unit(step, c, shaped_of=None):
        def put(d, at, value):
            mix[d, c, pl.ds(at, ROWS, stride=PITCH), :] = value

        def fresh(n):
            return shape_rows(co_t[c], bas.at[step], tes.at[step], n)

        skin_rows(step, shaped_of or fresh, [po_t[d, c] for d in range(3)], wv.at[step], put)

    def early(c):
        wide_move(0, n_batch - 1, slice(c * ROWS, (c + 1) * ROWS)).wait_recv()
        turn(c)
        unit(0, c, lambda n: [early_shape[c, n, e] for e in range(3)])

    order = (2 - odd, 1 + odd)
    for at in range(3 * chunks + 1):
        for (slot, piece), kinds in takes_before(at, chunks, count):
            take(slot, piece, kinds)
        turn_of, c = at // chunks, at % chunks
        if (turn_of, c) in ((0, chunks - 1), (1, chunks - 2)):
            got(order[turn_of], (0, 1))
            place_weights(wes.at[order[turn_of]], n_batch, wv.at[order[turn_of]])
        if (turn_of, c) == (2, chunks - 2):
            got(LAST, (0, 1))
            place_weights(wes.at[LAST], n_batch, wv_last)
            for i in range(n_batch - 1):
                wide_move(i, 1, slice(0, chars)).wait_send()
            for where in (1, 2):
                for copy in all_pieces(where, bl_send, bl_recv, 1):
                    copy.wait_send()
        if turn_of == 0:
            early(c)
        if turn_of > 0 and c == 0:
            got(order[turn_of - 1] if turn_of < 3 else LAST, (2,))
        if 0 < turn_of < 3:
            unit(order[turn_of - 1], c)

    for slot in (2, 1, 3):
        for copy in all_pieces(slot - 1, fw_send, fw_recv, slot):
            copy.wait_send()

    @pl.when(odd == 0)
    def _():
        for where in (0, 3):
            for c in all_pieces(where, bl_send, bl_recv, 1):
                c.wait_send()


def front(n_blk, n_batch, coefficients, transforms, basis, template, weights):
    comps, jl, total = transforms.shape
    chars = total // n_batch
    chunks = chars // ROWS
    k = coefficients.shape[0]
    verts = weights.shape[1]
    joints = weights.shape[0]
    hop = STEPS - 1
    assert n_blk % 2 == 0 and n_blk > STEPS and n_batch % 2 == 0 and STEPS == 4
    assert chars % ROWS == 0 and k <= LANES and comps == 12
    assert joints == n_batch * jl and 4 * joints <= LANES
    sems = 3 * -(-k // CUT) + 2
    dma = pltpu.SemaphoreType.DMA
    any_spec = pl.BlockSpec(memory_space=pl.ANY)
    vmem_spec = pl.BlockSpec(memory_space=pltpu.VMEM)
    inputs = [
        pltpu.with_memory_space_constraint(a, pltpu.HBM)
        for a in (coefficients, transforms, basis, template, weights)
    ]
    return pl.pallas_call(
        functools.partial(front_kernel, n_blk, n_batch),
        out_shape=(
            pltpu.VMEM((3, chunks, ROWS * PITCH, LANES), F32),
            pltpu.VMEM((chunks, ROWS, LANES), BF16),
            pltpu.VMEM((3, chunks, ROWS, LANES), BF16),
            pltpu.VMEM((STEPS,) + basis.shape, BF16),
            pltpu.VMEM((STEPS,) + template.shape, BF16),
            pltpu.VMEM((4, LANES, verts), BF16),
        ),
        in_specs=[any_spec] * 5,
        out_specs=(vmem_spec,) * 6,
        scratch_shapes=[
            pltpu.VMEM((k, chars), BF16),
            pltpu.VMEM(transforms.shape, BF16),
            pltpu.VMEM((n_batch - 1, 3, 4 * jl, chars), BF16),
            pltpu.VMEM((n_batch, 3, 4 * jl, chars), BF16),
            pltpu.VMEM((STEPS,) + weights.shape, BF16),
            pltpu.VMEM((hop, 4, LANES, verts), BF16),
            pltpu.VMEM((chunks, verts // WIDE, 3, ROWS, WIDE), F32),
            dma((n_batch - 1,)), dma((chunks,)),
            dma((hop + 1, 3)), dma((hop, sems)), dma((hop, 3)), dma((hop, 3)), dma((5,)),
        ],
        compiler_params=pltpu.CompilerParams(
            collective_id=0, has_side_effects=True, vmem_limit_bytes=20 << 20
        ),
        cost_estimate=pl.CostEstimate(flops=0, bytes_accessed=20 << 20, transcendentals=0),
        name="front",
    )(*inputs)


def back_kernel(mix_in, co_t, po_t, bas, tes, wv, out_ref, mix, staged, sem):
    chunks = co_t.shape[0]
    part = ROWS // PARTS

    def send(c, p=None):
        low, size = (0, ROWS) if p is None else (p * part, part)
        return pltpu.make_async_copy(
            staged.at[c, pl.ds(low, size)], out_ref.at[pl.ds(c * ROWS + low, size)], sem.at[c, p or 0]
        )

    def pack(c, p):
        for r in range(p * part, (p + 1) * part):
            for d in range(3):
                low = mix[d, c, pl.ds(r * PITCH, 8, stride=2), :]
                high = mix[d, c, pl.ds(r * PITCH + 1, 8, stride=2), :]
                staged[c, r, d] = jnp.concatenate([low, high], axis=0).astype(BF16)

    for c in range(chunks):
        def put(d, at, value):
            mix[d, c, pl.ds(at, ROWS, stride=PITCH), :] = value

        skin_rows(
            LAST, lambda n: shape_rows(co_t[c], bas.at[LAST], tes.at[LAST], n),
            [po_t[d, c] for d in range(3)], wv, put,
        )
        if c > 0:
            for p in range(PARTS):
                pack(c - 1, p)
            send(c - 1).start()
    for p in range(PARTS):
        pack(chunks - 1, p)
        send(chunks - 1, p).start()
    for c in range(chunks - 1):
        send(c).wait()
    for p in range(PARTS):
        send(chunks - 1, p).wait()


def back(mix, co_t, po_t, bas, tes, wv):
    chunks = co_t.shape[0]
    chars = chunks * ROWS
    verts = wv.shape[2]
    group = (verts // LANES) * STEPS
    any_spec = pl.BlockSpec(memory_space=pl.ANY)
    vmem_spec = pl.BlockSpec(memory_space=pltpu.VMEM)
    out, _ = pl.pallas_call(
        back_kernel,
        out_shape=(
            jax.ShapeDtypeStruct((chars, 3, group, LANES), BF16),
            pltpu.VMEM(mix.shape, F32),
        ),
        in_specs=[vmem_spec] * 6,
        out_specs=(any_spec, vmem_spec),
        input_output_aliases={0: 1},
        scratch_shapes=[
            pltpu.VMEM((chunks, ROWS, 3, group, LANES), BF16),
            pltpu.SemaphoreType.DMA((chunks, PARTS)),
        ],
        compiler_params=pltpu.CompilerParams(vmem_limit_bytes=20 << 20),
        name="back",
    )(mix, co_t, po_t, bas, tes, wv)
    out = out.reshape(chars, 3, verts // LANES, STEPS, LANES)
    return out.transpose(0, 3, 1, 2, 4).reshape(chars, STEPS, 3, verts)


def solution(mesh):
    n_blk, n_batch = mesh.shape["blk"], mesh.shape["batch"]

    def per_device(coefficients, transforms, basis, template, skin_weights):
        basis = jnp.transpose(basis, (1, 0, 2))
        return back(*front(
            n_blk, n_batch, coefficients, transforms, basis, template, skin_weights
        ))

    in_specs = (
        P(None, ("blk", "batch")),
        P(None, "batch", "blk"),
        P(None, None, "blk"),
        P(None, "blk"),
        P(None, "blk"),
    )
    out_specs = P(("blk", "batch"), None, None, None)
    return jax.shard_map(
        per_device, mesh=mesh, in_specs=in_specs, out_specs=out_specs, check_vma=False
    )
```

```python
import functools
import jax
import jax.numpy as jnp
from jax import lax
from jax.experimental import pallas as pl
from jax.experimental.pallas import tpu as pltpu
from jax.sharding import PartitionSpec as P

STEPS = 4
LANES = 128
WIDE = 256
ROWS = 128
PITCH = 20
PARTS = 4
CUT = 40
BF16 = jnp.bfloat16
F32 = jnp.float32
LAST = STEPS - 1


def place_weights(raw, n_batch, wv):
    joints, verts = raw.shape
    jl = joints // n_batch
    w = raw[...].astype(F32)
    w = (w / jnp.sum(w, axis=0, keepdims=True)).astype(BF16).astype(F32)
    for q in range(4):
        parts = []
        for i in range(n_batch):
            if q > 0:
                parts.append(jnp.zeros((q * jl, verts), F32))
            parts.append(w[i * jl:(i + 1) * jl])
            if q < 3:
                parts.append(jnp.zeros(((3 - q) * jl, verts), F32))
        if 4 * joints < LANES:
            parts.append(jnp.zeros((LANES - 4 * joints, verts), F32))
        wv[q] = jnp.concatenate(parts, axis=0).astype(BF16)


def shape_rows(coefs, basis, te, n):
    k = basis.shape[1]
    cols = slice(n * WIDE, (n + 1) * WIDE)
    return [
        jnp.dot(coefs[:, :k], basis[e, :, cols], preferred_element_type=F32) + te[e:e + 1, cols].astype(F32)
        for e in range(3)
    ]


def skin_rows(step, shaped_of, poses, wv, put):
    verts = wv.shape[2]
    for n in range(verts // WIDE):
        cols = slice(n * WIDE, (n + 1) * WIDE)
        shaped = shaped_of(n)
        for d in range(3):
            total = jnp.dot(poses[d], wv[3, :, cols], preferred_element_type=F32)
            for e in range(3):
                total = total + shaped[e] * jnp.dot(poses[d], wv[e, :, cols], preferred_element_type=F32)
            for h in range(WIDE // LANES):
                t = n * (WIDE // LANES) + h
                put(d, 8 * (t % 2) + t // 2 + 2 * step, total[:, h * LANES:(h + 1) * LANES])


WHEN = {
    "even": {2: (0, 1, 2, 3, 4, 5), 1: (3, 4, 5, 6, 8, 8), 3: (12, 16, 16, 16, 16, 16)},
    "odd": {2: (0, 1, 1, 2, 3, 4), 1: (1, 2, 3, 4, 5, 5), 3: (8, 8, 10, 10, 12, 12)},
    "even wrap": {2: (4, 5, 5, 6, 6, 6), 1: (8, 8, 10, 10, 11, 11), 3: (12, 16, 16, 16, 16, 16)},
    "odd wrap": {2: (3, 4, 5, 6, 6, 6), 1: (1, 2, 3, 4, 5, 5), 3: (12, 16, 16, 16, 16, 16)},
}


def takes_before(at, chunks, count):
    found = {}
    for kind, slots in WHEN.items():
        for slot, times in slots.items():
            for p in range(count):
                if times[p * 6 // count] * chunks // 6 == at:
                    found.setdefault((slot, p), []).append(kind)
    return sorted(found.items(), key=lambda item: ((2, 1, 3).index(item[0][0]), item[0][1]))


def front_kernel(
    n_blk, n_batch, co_ref, tr_ref, ba_ref, te_ref, we_ref,
    mix, co_t, po_t, bas, tes, wv_last,
    cov, stage, packed, trv, wes, wv, early_shape,
    tr_send, tr_recv, bl_send, bl_recv, fw_send, fw_recv, own_sem,
):
    blk, bat = lax.axis_index("blk"), lax.axis_index("batch")
    sibling = bat + 1 - 2 * lax.rem(bat, 2)
    odd = lax.rem(blk, 2)
    pair = blk + 1 - 2 * odd
    after = lax.rem(blk + 2, n_blk)
    before = lax.rem(blk + n_blk - 2, n_blk)
    chars = trv.shape[3]
    chunks = chars // ROWS
    jl = stage.shape[1]
    k = cov.shape[0]
    verts = bas.shape[3]
    half = verts // 2

    own = [
        pltpu.make_async_copy(we_ref, wes.at[0], own_sem.at[0]),
        pltpu.make_async_copy(te_ref, tes.at[0], own_sem.at[1]),
        pltpu.make_async_copy(ba_ref, bas.at[0], own_sem.at[2]),
        pltpu.make_async_copy(tr_ref, stage, own_sem.at[3]),
        pltpu.make_async_copy(co_ref, cov, own_sem.at[4]),
    ]

    partners = [lax.rem(bat + i, n_batch) for i in range(1, n_batch)]
    barrier = pltpu.get_barrier_semaphore()
    for q in partners:
        pl.semaphore_signal(barrier, inc=1, device_id={"blk": blk, "batch": q})
    for b in (pair, before):
        pl.semaphore_signal(barrier, inc=1, device_id={"blk": b, "batch": bat})
    for c in own:
        c.start()

    mine = pl.ds(pl.multiple_of(lax.rem(bat, 2) * half, LANES), half)
    pieces = []
    for e in range(3):
        for low in range(0, k, CUT):
            pieces.append([(bas, e, pl.ds(low, min(CUT, k - low)))])
    pieces[0] = [tes, wes] + pieces[0]
    count = len(pieces)

    def part(entry, slot):
        if isinstance(entry, tuple):
            return entry[0].at[slot, entry[1], entry[2], mine]
        return entry.at[slot, :, mine]

    def kind_of(piece, i):
        return i if piece == 0 else 2

    def hop(slot_from, slot_to, piece, where, send, recv, target, shared=False):
        made = []
        for i, entry in enumerate(pieces[piece]):
            kind = kind_of(piece, i)
            at = kind if shared or kind < 2 else piece + 2
            made.append(pltpu.make_async_remote_copy(
                src_ref=part(entry, slot_from), dst_ref=part(entry, slot_to),
                send_sem=send.at[where, kind], recv_sem=recv.at[slot_to - 1, at],
                device_id={"blk": target[0], "batch": target[1]},
            ))
        return made

    def all_pieces(where, send, recv, slot):
        return [
            pltpu.make_async_remote_copy(
                src_ref=ref, dst_ref=ref, send_sem=send.at[where, kind], recv_sem=recv.at[slot - 1, kind],
                device_id={"blk": blk, "batch": sibling},
            )
            for kind, ref in enumerate(
                (tes.at[slot, :, mine], wes.at[slot, :, mine], bas.at[slot, :, :, mine])
            )
        ]

    def start(copies):
        for c in copies:
            c.start()

    def first_hop(piece):
        return hop(0, 2, piece, 1, bl_send, bl_recv, (after, bat))

    def to_odd(piece):
        return hop(0, 1, piece, 0, bl_send, bl_recv, (pair, bat))

    def across(piece):
        return hop(2, 3 - 2 * odd, piece, 2, bl_send, bl_recv, (pair, bat))

    def onward(piece):
        return hop(1, 3, piece, 3, bl_send, bl_recv, (after, bat))

    def share(slot, piece):
        return hop(slot, slot, piece, slot - 1, fw_send, fw_recv, (blk, sibling), shared=True)

    wrap = blk < 2
    is_kind = {
        "even": jnp.logical_and(odd == 0, jnp.logical_not(wrap)),
        "odd": jnp.logical_and(odd == 1, jnp.logical_not(wrap)),
        "even wrap": jnp.logical_and(odd == 0, wrap),
        "odd wrap": jnp.logical_and(odd == 1, wrap),
    }

    def take(slot, piece, kinds):
        def body():
            for c in hop(slot, slot, piece, slot - 1, bl_send, bl_recv, (pair, bat)):
                c.wait_recv()
            if slot == 2:
                start(across(piece))
            if slot == 1:
                @pl.when(odd == 0)
                def _():
                    start(onward(piece))
            start(share(slot, piece))

        if len(kinds) == len(is_kind):
            body()
        else:
            pl.when(functools.reduce(jnp.logical_or, [is_kind[x] for x in kinds]))(body)

    def got(slot, kinds):
        copies = all_pieces(slot - 1, fw_send, fw_recv, slot)
        for kind in kinds:
            copies[kind].wait_recv()

    moves = [[] for _ in range(chunks)]
    for c in range(chunks):
        for i, q in enumerate(partners):
            moves[c].append(pltpu.make_async_remote_copy(
                src_ref=packed.at[i, :, :, pl.ds(c * ROWS, ROWS)],
                dst_ref=trv.at[bat, :, :, pl.ds(c * ROWS, ROWS)],
                send_sem=tr_send.at[i], recv_sem=tr_recv.at[c],
                device_id={"blk": blk, "batch": q},
            ))

    def wide_move(i, count, cols):
        ref = trv.at[pl.ds(0, count), :, :, cols]
        return pltpu.make_async_remote_copy(
            src_ref=ref, dst_ref=ref, send_sem=tr_send.at[i], recv_sem=tr_recv.at[cols.start // ROWS],
            device_id={"blk": blk, "batch": partners[i]},
        )


    for c in own[:3]:
        c.wait()
    pl.semaphore_wait(barrier, len(partners) + 2)
    for p in range(count):
        start(first_hop(p))

    @pl.when(odd == 0)
    def _():
        for p in range(count):
            start(to_odd(p))

    own[3].wait()
    for i, q in enumerate(partners + [bat]):
        for c in range(chunks):
            cols = pl.ds(pl.multiple_of(q * chars + c * ROWS, LANES), ROWS)
            for d in range(3):
                rows = jnp.concatenate(
                    [stage[4 * d + e, :, cols].astype(F32) for e in range(4)], axis=0
                ).astype(BF16)
                if i < n_batch - 1:
                    packed[i, d, :, c * ROWS:(c + 1) * ROWS] = rows
                else:
                    trv[bat, d, :, c * ROWS:(c + 1) * ROWS] = rows

    for c in range(chunks):
        start(moves[c])

    place_weights(wes.at[0], n_batch, wv.at[0])
    own[4].wait()
    rest = jnp.zeros((LANES - k, ROWS), F32)
    for c in range(chunks):
        block = jnp.concatenate([cov[:, c * ROWS:(c + 1) * ROWS].astype(F32), rest], axis=0)
        co_t[c] = block.T.astype(BF16)
    for c in range(chunks):
        for n in range(verts // WIDE):
            for e, value in enumerate(shape_rows(co_t[c], bas.at[0], tes.at[0], n)):
                early_shape[c, n, e] = value

    def turn(c):
        for d in range(3):
            parts = [trv[i, d, :, c * ROWS:(c + 1) * ROWS].astype(F32) for i in range(n_batch)]
            if 4 * n_batch * jl < LANES:
                parts.append(jnp.zeros((LANES - 4 * n_batch * jl, ROWS), F32))
            po_t[d, c] = jnp.concatenate(parts, axis=0).T.astype(BF16)

    def unit(step, c, shaped_of=None):
        def put(d, at, value):
            mix[d, c, pl.ds(at, ROWS, stride=PITCH), :] = value

        def fresh(n):
            return shape_rows(co_t[c], bas.at[step], tes.at[step], n)

        skin_rows(step, shaped_of or fresh, [po_t[d, c] for d in range(3)], wv.at[step], put)

    def early(c):
        wide_move(0, n_batch - 1, slice(c * ROWS, (c + 1) * ROWS)).wait_recv()
        turn(c)
        unit(0, c, lambda n: [early_shape[c, n, e] for e in range(3)])

    order = (2 - odd, 1 + odd)
    for at in range(3 * chunks + 1):
        for (slot, piece), kinds in takes_before(at, chunks, count):
            take(slot, piece, kinds)
        turn_of, c = at // chunks, at % chunks
        if (turn_of, c) in ((0, chunks - 1), (1, chunks - 2)):
            got(order[turn_of], (0, 1))
            place_weights(wes.at[order[turn_of]], n_batch, wv.at[order[turn_of]])
        if (turn_of, c) == (2, chunks - 2):
            got(LAST, (0, 1))
            place_weights(wes.at[LAST], n_batch, wv_last)
            for i in range(n_batch - 1):
                wide_move(i, 1, slice(0, chars)).wait_send()
            for where in (1, 2):
                for copy in all_pieces(where, bl_send, bl_recv, 1):
                    copy.wait_send()
        if turn_of == 0:
            early(c)
        if turn_of > 0 and c == 0:
            got(order[turn_of - 1] if turn_of < 3 else LAST, (2,))
        if 0 < turn_of < 3:
            unit(order[turn_of - 1], c)

    for slot in (2, 1, 3):
        for copy in all_pieces(slot - 1, fw_send, fw_recv, slot):
            copy.wait_send()

    @pl.when(odd == 0)
    def _():
        for where in (0, 3):
            for c in all_pieces(where, bl_send, bl_recv, 1):
                c.wait_send()


def front(n_blk, n_batch, coefficients, transforms, basis, template, weights):
    comps, jl, total = transforms.shape
    chars = total // n_batch
    chunks = chars // ROWS
    k = coefficients.shape[0]
    verts = weights.shape[1]
    joints = weights.shape[0]
    hop = STEPS - 1
    assert n_blk % 2 == 0 and n_blk > STEPS and n_batch % 2 == 0 and STEPS == 4
    assert chars % ROWS == 0 and k <= LANES and comps == 12
    assert joints == n_batch * jl and 4 * joints <= LANES
    sems = 3 * -(-k // CUT) + 2
    dma = pltpu.SemaphoreType.DMA
    any_spec = pl.BlockSpec(memory_space=pl.ANY)
    vmem_spec = pl.BlockSpec(memory_space=pltpu.VMEM)
    inputs = [
        pltpu.with_memory_space_constraint(a, pltpu.HBM)
        for a in (coefficients, transforms, basis, template, weights)
    ]
    return pl.pallas_call(
        functools.partial(front_kernel, n_blk, n_batch),
        out_shape=(
            pltpu.VMEM((3, chunks, ROWS * PITCH, LANES), F32),
            pltpu.VMEM((chunks, ROWS, LANES), BF16),
            pltpu.VMEM((3, chunks, ROWS, LANES), BF16),
            pltpu.VMEM((STEPS,) + basis.shape, BF16),
            pltpu.VMEM((STEPS,) + template.shape, BF16),
            pltpu.VMEM((4, LANES, verts), BF16),
        ),
        in_specs=[any_spec] * 5,
        out_specs=(vmem_spec,) * 6,
        scratch_shapes=[
            pltpu.VMEM((k, chars), BF16),
            pltpu.VMEM(transforms.shape, BF16),
            pltpu.VMEM((n_batch - 1, 3, 4 * jl, chars), BF16),
            pltpu.VMEM((n_batch, 3, 4 * jl, chars), BF16),
            pltpu.VMEM((STEPS,) + weights.shape, BF16),
            pltpu.VMEM((hop, 4, LANES, verts), BF16),
            pltpu.VMEM((chunks, verts // WIDE, 3, ROWS, WIDE), F32),
            dma((n_batch - 1,)), dma((chunks,)),
            dma((hop + 1, 3)), dma((hop, sems)), dma((hop, 3)), dma((hop, 3)), dma((5,)),
        ],
        compiler_params=pltpu.CompilerParams(
            collective_id=0, has_side_effects=True, vmem_limit_bytes=20 << 20
        ),
        cost_estimate=pl.CostEstimate(flops=0, bytes_accessed=20 << 20, transcendentals=0),
        name="front",
    )(*inputs)


def back_kernel(mix_in, co_t, po_t, bas, tes, wv, out_ref, mix, staged, sem):
    chunks = co_t.shape[0]
    part = ROWS // PARTS

    def send(c, p=None):
        low, size = (0, ROWS) if p is None else (p * part, part)
        return pltpu.make_async_copy(
            staged.at[c, pl.ds(low, size)], out_ref.at[pl.ds(c * ROWS + low, size)], sem.at[c, p or 0]
        )

    def pack(c, p):
        for r in range(p * part, (p + 1) * part):
            for d in range(3):
                low = mix[d, c, pl.ds(r * PITCH, 8, stride=2), :]
                high = mix[d, c, pl.ds(r * PITCH + 1, 8, stride=2), :]
                staged[c, r, d] = jnp.concatenate([low, high], axis=0).astype(BF16)

    for c in range(chunks):
        def put(d, at, value):
            mix[d, c, pl.ds(at, ROWS, stride=PITCH), :] = value

        skin_rows(
            LAST, lambda n: shape_rows(co_t[c], bas.at[LAST], tes.at[LAST], n),
            [po_t[d, c] for d in range(3)], wv, put,
        )
        if c > 0:
            for p in range(PARTS):
                pack(c - 1, p)
            send(c - 1).start()
    for p in range(PARTS):
        pack(chunks - 1, p)
        send(chunks - 1, p).start()
    for c in range(chunks - 1):
        send(c).wait()
    for p in range(PARTS):
        send(chunks - 1, p).wait()


def back(mix, co_t, po_t, bas, tes, wv):
    chunks = co_t.shape[0]
    chars = chunks * ROWS
    verts = wv.shape[2]
    group = (verts // LANES) * STEPS
    any_spec = pl.BlockSpec(memory_space=pl.ANY)
    vmem_spec = pl.BlockSpec(memory_space=pltpu.VMEM)
    out, _ = pl.pallas_call(
        back_kernel,
        out_shape=(
            jax.ShapeDtypeStruct((chars, 3, group, LANES), BF16),
            pltpu.VMEM(mix.shape, F32),
        ),
        in_specs=[vmem_spec] * 6,
        out_specs=(any_spec, vmem_spec),
        input_output_aliases={0: 1},
        scratch_shapes=[
            pltpu.VMEM((chunks, ROWS, 3, group, LANES), BF16),
            pltpu.SemaphoreType.DMA((chunks, PARTS)),
        ],
        compiler_params=pltpu.CompilerParams(vmem_limit_bytes=20 << 20),
        name="back",
    )(mix, co_t, po_t, bas, tes, wv)
    out = out.reshape(chars, 3, verts // LANES, STEPS, LANES)
    return out.transpose(0, 3, 1, 2, 4).reshape(chars, STEPS, 3, verts)


def solution(mesh):
    n_blk, n_batch = mesh.shape["blk"], mesh.shape["batch"]

    def per_device(coefficients, transforms, basis, template, skin_weights):
        basis = jnp.transpose(basis, (1, 0, 2))
        return back(*front(
            n_blk, n_batch, coefficients, transforms, basis, template, skin_weights
        ))

    in_specs = (
        P(None, ("blk", "batch")),
        P(None, "batch", "blk"),
        P(None, None, "blk"),
        P(None, "blk"),
        P(None, "blk"),
    )
    out_specs = P(("blk", "batch"), None, None, None)
    return jax.shard_map(
        per_device, mesh=mesh, in_specs=in_specs, out_specs=out_specs, check_vma=False
    )
```
